32 devices in a mesh: seq: 8 (over z, x), head: 4 (over y, core).
Axes of the slice: x: 2, y: 2, z: 4, core: 2. Of those that a mesh axis runs over, the one named last changes fastest.
Arguments:
- tokens: bfloat16 [8192, 2048], P('seq'), may hold values from -6 to 6
- owner_slot: int32 [8192], P('seq'), may hold values from 0 to 2047, as said below
- w_in: bfloat16 [8, 2048, 4096], P('seq', None, 'head'), as said below
- w_bc: bfloat16 [2048, 256], replicated, may hold values from -0.125 to 0.125
- w_dt: bfloat16 [2048, 32], P(None, 'head'), may hold values from -0.125 to 0.125
- conv_x: float32 [4, 2048], P(None, 'head'), may hold values from -3 to 3
- conv_bc: float32 [4, 256], replicated, may hold values from -3 to 3
- dt_bias: float32 [32], P('head'), may hold values from -1 to 1
- decay_rate: float32 [32], P('head'), may hold values from 2e-06 to 0.1
- d_skip: float32 [32], P('head'), may hold values from 0.5 to 2
- norm_gain: float32 [2048], P('head'), may hold values from 0.5 to 1.5
Outputs:
- normed: bfloat16 [8192, 2048], P('seq', 'head')
The draws below stay inside these ranges and needn't reach their ends.
Inputs may be any that keep to these rules, and one draw needn't show every extreme that they name: Within each block of 1024 tokens the values are distinct; the owner owner_slot // 256 gets at most 256 tokens of one block, and in every draw one owner gets exactly 256 tokens of every block. The token's modality is the owner's index modulo 3. Owner o holds the projection of modality o % 3: w_in[o] equals w_in[o % 3].
All inputs are finite; a program needn't handle non-finite values.
Results may differ from the reference program's by a relative error of at most 0.0054.
Values may be sent and summed in bfloat16 or wider, within the bound.
A program may use at most 128 MiB of HBM per device.

```python
import math
import jax
import jax.numpy as jnp
from jax import lax

D = 2048
HDIM = 64
NSTATE = 128
MODS = 3
KCONV = 4
QB = 256
TOK_DEV = 1024
TOKENS = 8192
HEADS = 32
INNER = 2048
CAP = 256
N_SEQ = 8


def owner_plan(key):
    slot_total = N_SEQ * CAP
    slot_ids = jnp.arange(slot_total, dtype=jnp.int32)
    owners = slot_ids // CAP
    full_owner = jax.random.randint(jax.random.fold_in(key, 1), (), 0, N_SEQ)
    busy_modality = jax.random.randint(jax.random.fold_in(key, 2), (), 0, MODS)

    def one_block(block_key):
        random_part = jax.random.randint(jax.random.fold_in(block_key, 3), (slot_total,), 0, 4096)
        scores = random_part + jnp.where(owners == full_owner, 16384, 0) + jnp.where(owners % MODS == busy_modality, 2048, 0)
        ranked = scores * slot_total + slot_ids
        picked = jnp.argsort(-ranked)[:TOK_DEV].astype(jnp.int32)
        modality = picked // CAP % MODS
        order_rank = jax.random.permutation(jax.random.fold_in(block_key, 4), MODS)
        jitter = jax.random.randint(jax.random.fold_in(block_key, 5), (TOK_DEV,), 0, 1024)
        sort_keys = (order_rank[modality] * 1024 + jitter) * slot_total + picked
        return picked[jnp.argsort(sort_keys)].astype(jnp.int32)
    blocks = jax.vmap(one_block)(jax.random.split(jax.random.fold_in(key, 9), N_SEQ))
    return blocks.reshape(N_SEQ * TOK_DEV)


def draw_owner_slot(key, part):
    return owner_plan(key)


def draw_w_in(key, part):
    modal_base = (jax.random.normal(jax.random.fold_in(key, 7), (MODS, D, 2 * INNER), jnp.float32) * D ** (-0.5)).astype(jnp.bfloat16)
    return modal_base[jnp.arange(N_SEQ) % MODS]


def block_scale(own_key, extent, shards, least, largest):
    def one(dim, parts):
        heights = jax.random.uniform(jax.random.fold_in(jax.random.fold_in(own_key, 6), dim), (parts,), jnp.float32, least / len(shards), largest / len(shards))
        return jnp.repeat(jnp.exp(heights), extent[dim] // parts).reshape((-1,) + (1,) * (len(extent) - dim - 1))

    loudness = one(*shards[0])
    for cut in shards[1:]:
        loudness = loudness * one(*cut)
    return loudness


def gaussian(key, shape, spread, bound, cuts=(), held_as=jnp.bfloat16):
    entries = jax.random.normal(key, shape, jnp.float32) * spread
    if len(cuts) > 0:
        entries = block_scale(key, shape, cuts, -0.22, 0.18) * entries
    return jnp.clip(entries, min=-bound, max=bound).astype(held_as)


def setup_inputs(seed: int = 0) -> dict:
    streams_of = jax.random.split(jax.random.key(seed), 12)
    tokens = gaussian(streams_of[0], (TOKENS, D), 1.0, 6.0, ((0, 8),))
    owner_slot = draw_owner_slot(jax.random.fold_in(streams_of[11], 71), 0)
    w_in = draw_w_in(jax.random.fold_in(streams_of[11], 71), 0)
    w_bc = gaussian(streams_of[3], (D, 2 * NSTATE), D ** -0.5, 0.125)
    w_dt = gaussian(streams_of[4], (D, HEADS), D ** -0.5, 0.125, ((1, 4),))
    conv_x = gaussian(streams_of[5], (KCONV, INNER), KCONV ** -0.5, 3.0, ((1, 4),), jnp.float32)
    conv_bc = gaussian(streams_of[6], (KCONV, 2 * NSTATE), KCONV ** -0.5, 3.0, (), jnp.float32)
    dt_bias = jnp.clip(jax.random.uniform(streams_of[7], (HEADS,), jnp.float32, -1.0, 1.0) * block_scale(streams_of[7], (HEADS,), ((0, 4),), -0.4, 0.0), -1.0, 1.0)
    decay_rate = jnp.clip(jnp.exp(math.log(0.1) - 10.819778 * jax.random.uniform(streams_of[8], (HEADS,), jnp.float32) ** block_scale(streams_of[8], (HEADS,), ((0, 4),), -0.2, 0.2)), 1.9999999949504854e-06, 0.1)
    d_skip = jnp.clip(0.5 + 1.5 * jax.random.uniform(streams_of[9], (HEADS,), jnp.float32) ** block_scale(streams_of[9], (HEADS,), ((0, 4),), -0.2, 0.2), 0.5, 2.0)
    norm_gain = jnp.clip(1.0 + 0.1 * jax.random.normal(streams_of[10], (INNER,), jnp.float32), 0.5, 1.5)
    return {"tokens": tokens, "owner_slot": owner_slot, "w_in": w_in, "w_bc": w_bc, "w_dt": w_dt, "conv_x": conv_x, "conv_bc": conv_bc, "dt_bias": dt_bias, "decay_rate": decay_rate, "d_skip": d_skip, "norm_gain": norm_gain}


EPSILON = 1e-05

def causal_conv(values, rim, weights):
    kernel_width = weights.shape[0]
    joined = jnp.concatenate([rim, values]).astype(jnp.float32)
    length = values.shape[0]
    summed = jnp.zeros(values.shape, jnp.float32)
    for offset in range(kernel_width):
        summed = summed + weights[offset] * joined[offset:offset + length]
    return summed

def block_terms(x_blk, b_blk, c_blk, dt_blk, log_blk):
    length = x_blk.shape[0]
    cumulative = jnp.cumsum(log_blk, axis=0)
    scores = jnp.dot(c_blk, b_blk.T, preferred_element_type=jnp.float32)
    log_gaps = cumulative[:, None, :] - cumulative[None, :, :]
    row_index = lax.broadcasted_iota(jnp.int32, (length, length), 0)
    col_index = lax.broadcasted_iota(jnp.int32, (length, length), 1)
    causal = (row_index >= col_index)[:, :, None]
    mixing = (scores[:, :, None] * jnp.exp(jnp.where(causal, log_gaps, -jnp.inf)) * dt_blk[None, :, :]).astype(jnp.bfloat16)
    inside = jnp.einsum('ijh,jhp->ihp', mixing.astype(jnp.float32), x_blk.astype(jnp.float32))
    to_end = jnp.exp(cumulative[-1:, :] - cumulative) * dt_blk
    weighted = (x_blk.astype(jnp.float32) * to_end[:, :, None]).astype(jnp.bfloat16)
    block_state = jnp.einsum('jhp,jn->hpn', weighted.astype(jnp.float32), b_blk.astype(jnp.float32))
    return (inside, block_state, cumulative)

def reference(tokens, owner_slot, w_in, w_bc, w_dt, conv_x, conv_bc, dt_bias, decay_rate, d_skip, norm_gain):
    modality = owner_slot // CAP % MODS
    projected = jnp.zeros((TOKENS, 2 * INNER), jnp.float32)
    for which in range(MODS):
        product = jnp.dot(tokens, w_in[which], preferred_element_type=jnp.float32)
        projected = jnp.where((modality == which)[:, None], product, projected)
    projected = projected.astype(jnp.bfloat16).reshape(TOKENS, HEADS, 2, HDIM)
    x_raw = projected[:, :, 0, :].reshape(TOKENS, INNER)
    z_gate = projected[:, :, 1, :].reshape(TOKENS, INNER)
    bc_raw = jnp.dot(tokens, w_bc, preferred_element_type=jnp.float32).astype(jnp.bfloat16)
    dt_raw = jnp.dot(tokens, w_dt, preferred_element_type=jnp.float32)
    x_conv = jax.nn.silu(causal_conv(x_raw, jnp.zeros((KCONV - 1, INNER), jnp.bfloat16), conv_x)).astype(jnp.bfloat16)
    bc_conv = jax.nn.silu(causal_conv(bc_raw, jnp.zeros((KCONV - 1, 2 * NSTATE), jnp.bfloat16), conv_bc)).astype(jnp.bfloat16)
    steps_dt = jax.nn.softplus(dt_raw + dt_bias)
    log_decay = -steps_dt * decay_rate
    block_total = TOKENS // QB
    pieces = (x_conv.reshape(block_total, QB, HEADS, HDIM), bc_conv[:, :NSTATE].reshape(block_total, QB, NSTATE), bc_conv[:, NSTATE:].reshape(block_total, QB, NSTATE), steps_dt.reshape(block_total, QB, HEADS), log_decay.reshape(block_total, QB, HEADS))

    def advance(states, block):
        x_blk, b_blk, c_blk, dt_blk, log_blk = block
        inside, block_state, cumulative = block_terms(x_blk, b_blk, c_blk, dt_blk, log_blk)
        outside = jnp.exp(cumulative)[:, :, None] * jnp.einsum('in,hpn->ihp', c_blk.astype(jnp.float32), states, precision=lax.Precision.HIGHEST)
        result = inside + outside + d_skip[None, :, None] * x_blk.astype(jnp.float32)
        states = states * jnp.exp(cumulative[-1])[:, None, None] + block_state
        return (states, result)
    start_state = jnp.zeros((HEADS, HDIM, NSTATE), jnp.float32)
    final_state, outputs = lax.scan(advance, start_state, pieces)
    outputs = outputs.reshape(TOKENS, INNER)
    gated = outputs * jax.nn.silu(z_gate.astype(jnp.float32))
    mean_square = lax.optimization_barrier(jnp.mean(gated * gated, axis=1, keepdims=True))
    return (gated * lax.rsqrt(mean_square + EPSILON) * norm_gain).astype(jnp.bfloat16)
```

```python
import jax
import jax.numpy as jnp
from jax import lax
from jax.sharding import PartitionSpec as P

KCONV = 4
QB = 256
MODS = 3


EPSILON = 1e-05
PRECISE = lax.Precision.HIGHEST


def passed_along(value, axis, steps):
    count = lax.axis_size(axis)
    initial, last = (max(0, -steps), min(count, count - steps))
    return lax.ppermute(value, axis, [(source, source + steps) for source in range(initial, last)])


def swapped(value, bit):
    count = lax.axis_size("seq")
    return lax.ppermute(value, "seq", [(source, source ^ bit) for source in range(count)])


def exchange_pair(halves):
    index = lax.axis_index("seq")
    orders = ((1, 2), (2, 1))
    firsts = [swapped(half, bits[0]) for half, bits in zip(halves, orders)]
    slots = []
    for half, got, bits in zip(halves, firsts, orders):
        partner = index ^ bits[1]
        wanted = MODS - partner % MODS - (partner ^ bits[0]) % MODS
        sent = jnp.where(index % MODS == wanted, half, got)
        slots.append((half, got, swapped(sent, bits[1])))
    return slots


def causal_conv(values, rim, weights):
    kernel_width = weights.shape[0]
    joined = jnp.concatenate([rim, values]).astype(jnp.float32)
    length = values.shape[0]
    summed = jnp.zeros(values.shape, jnp.float32)
    for offset in range(kernel_width):
        summed = summed + weights[offset] * joined[offset : offset + length]
    return summed


def block_terms(x_blk, b_blk, c_blk, dt_blk, log_blk):
    length = x_blk.shape[0]
    cumulative = jnp.cumsum(log_blk, axis=0)
    scores = jnp.dot(c_blk, b_blk.T, preferred_element_type=jnp.float32)
    log_gaps = cumulative[:, None, :] - cumulative[None, :, :]
    row_index = lax.broadcasted_iota(jnp.int32, (length, length), 0)
    col_index = lax.broadcasted_iota(jnp.int32, (length, length), 1)
    causal = (row_index >= col_index)[:, :, None]
    mixing = (
        scores[:, :, None] * jnp.exp(jnp.where(causal, log_gaps, -jnp.inf)) * dt_blk[None, :, :]
    ).astype(jnp.bfloat16)
    inside = jnp.einsum("ijh,jhp->ihp", mixing, x_blk, preferred_element_type=jnp.float32)
    to_end = jnp.exp(cumulative[-1:, :] - cumulative) * dt_blk
    weighted = (x_blk.astype(jnp.float32) * to_end[:, :, None]).astype(jnp.bfloat16)
    block_state = jnp.einsum("jhp,jn->hpn", weighted, b_blk, preferred_element_type=jnp.float32)
    return (inside, block_state, cumulative)


def per_device(
    tokens, owner_slot, w_in, w_bc, w_dt, conv_x, conv_bc, dt_bias, decay_rate, d_skip, norm_gain
):
    seq_count = lax.axis_size("seq")
    head_count = lax.axis_size("head")
    tok_rows = tokens.shape[0]
    width = tokens.shape[1]
    capacity = 2 * tok_rows // seq_count
    heads_here = dt_bias.shape[0]
    columns = w_in.shape[2]
    head_size = columns // (2 * heads_here)
    nstate = w_bc.shape[1] // 2
    own_index = lax.axis_index("seq")
    inner_here = heads_here * head_size
    half = inner_here // 2
    by_head = w_in[0].reshape(width, heads_here, 2, head_size)
    x_own = by_head[:, :, 0, :].reshape(width, inner_here)
    x_a, x_b = exchange_pair((x_own[:, :half], x_own[:, half:]))
    z_cols, x_a, x_b = lax.optimization_barrier((by_head[:, :, 1, :], x_a, x_b))
    z_own = z_cols.reshape(width, inner_here)
    z_a, z_b = exchange_pair((z_own[:, :half], z_own[:, half:]))
    modality = (owner_slot // capacity) % MODS

    def project(slots, bits):
        first = bits[0]
        own_mod = own_index % MODS
        next_mod = (own_index ^ first) % MODS
        products = [
            jnp.dot(tokens, slot, preferred_element_type=jnp.float32).astype(jnp.bfloat16)
            for slot in slots
        ]
        return jnp.where(
            (modality == own_mod)[:, None],
            products[0],
            jnp.where((modality == next_mod)[:, None], products[1], products[2]),
        )

    x_raw = jnp.concatenate([project(x_a, (1, 2)), project(x_b, (2, 1))], axis=1)
    z_gate = jnp.concatenate([project(z_a, (1, 2)), project(z_b, (2, 1))], axis=1)
    bc_raw = jnp.dot(tokens, w_bc, preferred_element_type=jnp.float32).astype(jnp.bfloat16)
    dt_raw = jnp.dot(tokens, w_dt, preferred_element_type=jnp.float32)
    x_rim, bc_rim = passed_along(
        (x_raw[tok_rows - KCONV + 1 :], bc_raw[tok_rows - KCONV + 1 :]), "seq", 1
    )
    x_conv = jax.nn.silu(causal_conv(x_raw, x_rim, conv_x)).astype(jnp.bfloat16)
    bc_conv = jax.nn.silu(causal_conv(bc_raw, bc_rim, conv_bc)).astype(jnp.bfloat16)
    steps_dt = jax.nn.softplus(dt_raw + dt_bias)
    log_decay = -steps_dt * decay_rate
    block_total = tok_rows // QB
    x_blocks = x_conv.reshape(block_total, QB, heads_here, head_size)
    b_blocks = bc_conv[:, :nstate].reshape(block_total, QB, nstate)
    c_blocks = bc_conv[:, nstate:].reshape(block_total, QB, nstate)
    inside, block_state, cumulative = jax.vmap(block_terms)(
        x_blocks,
        b_blocks,
        c_blocks,
        steps_dt.reshape(block_total, QB, heads_here),
        log_decay.reshape(block_total, QB, heads_here),
    )
    block_log = cumulative[:, -1, :]
    zero_state = jnp.zeros((heads_here, head_size, nstate), jnp.float32)

    def carry_local(states, pieces):
        state_here, log_here = pieces
        return (states * jnp.exp(log_here)[:, None, None] + state_here, states)

    device_state, entering_local = lax.scan(carry_local, zero_state, (block_state, block_log))
    prior_log = jnp.cumsum(block_log, axis=0) - block_log
    device_log = jnp.sum(block_log, axis=0)
    all_logs = lax.all_gather(device_log[None], "seq", axis=0, tiled=True)
    prefix = jnp.cumsum(all_logs, axis=0)
    own_prefix = lax.dynamic_index_in_dim(
        prefix, own_index, 0, keepdims=False
    ) - lax.dynamic_index_in_dim(all_logs, own_index, 0, keepdims=False)
    piece = lax.all_gather(device_state[None], "seq", axis=0, tiled=True)
    piece_rows = piece.shape[0]
    positions = jnp.arange(piece_rows, dtype=jnp.int32)
    log_gap = own_prefix[None, :] - prefix
    factor = jnp.exp(jnp.where((positions < own_index)[:, None], log_gap, -jnp.inf))
    incoming = jnp.einsum("khpn,kh->hpn", piece, factor, precision=PRECISE)
    entering = entering_local + incoming[None] * jnp.exp(prior_log)[:, :, None, None]
    outside = jnp.exp(cumulative)[..., None] * jnp.einsum(
        "bin,bhpn->bihp", c_blocks.astype(jnp.float32), entering, precision=PRECISE
    )
    outputs = inside + outside + d_skip[None, None, :, None] * x_blocks.astype(jnp.float32)
    outputs = outputs.reshape(tok_rows, heads_here * head_size)
    gated = outputs * jax.nn.silu(z_gate.astype(jnp.float32))
    squares = lax.psum(jnp.sum(gated * gated, axis=1), "head")
    inner_total = heads_here * head_size * head_count
    scaling = lax.rsqrt(squares / inner_total + EPSILON)
    return (gated * scaling[:, None] * norm_gain).astype(jnp.bfloat16)


def solution(mesh):
    return jax.shard_map(
        per_device,
        mesh=mesh,
        in_specs=(
            P("seq", None),
            P("seq"),
            P("seq", None, "head"),
            P(),
            P(None, "head"),
            P(None, "head"),
            P(),
            P("head"),
            P("head"),
            P("head"),
            P("head"),
        ),
        out_specs=P("seq", "head"),
        check_vma=False,
    )
```

```python
import jax
import jax.numpy as jnp
from jax import lax
from jax.sharding import PartitionSpec as P

KCONV = 4
QB = 256
MODS = 3


EPSILON = 1e-05
PRECISE = lax.Precision.HIGHEST


def passed_along(value, axis, steps):
    count = lax.axis_size(axis)
    initial, last = (max(0, -steps), min(count, count - steps))
    return lax.ppermute(value, axis, [(source, source + steps) for source in range(initial, last)])


def swapped(value, bit):
    count = lax.axis_size("seq")
    return lax.ppermute(value, "seq", [(source, source ^ bit) for source in range(count)])


def picked(weight, part, head_size, kind):
    columns = weight.shape[1] // 2
    source = lax.broadcasted_iota(jnp.int32, (columns, columns // 2), 0)
    target = lax.broadcasted_iota(jnp.int32, (columns, columns // 2), 1)
    wanted = (target // head_size) * 2 * head_size + kind * head_size + target % head_size
    chooser = (source == wanted).astype(jnp.bfloat16)
    chunk = weight[:, part * columns : (part + 1) * columns]
    return jnp.dot(chunk, chooser, preferred_element_type=jnp.float32).astype(jnp.bfloat16)


def split_three(value):
    high = lax.reduce_precision(value, 8, 7)
    middle = lax.reduce_precision(value - high, 8, 7)
    return high, middle, value - high - middle


def exchange_pair(halves):
    index = lax.axis_index("seq")
    orders = ((1, 2), (2, 1))
    firsts = [swapped(half, bits[0]) for half, bits in zip(halves, orders)]
    slots = []
    for half, got, bits in zip(halves, firsts, orders):
        partner = index ^ bits[1]
        wanted = MODS - partner % MODS - (partner ^ bits[0]) % MODS
        sent = jnp.where(index % MODS == wanted, half, got)
        slots.append((half, got, swapped(sent, bits[1])))
    return slots


def causal_conv(values, rim, weights):
    kernel_width = weights.shape[0]
    joined = jnp.concatenate([rim, values]).astype(jnp.float32)
    length = values.shape[0]
    summed = jnp.zeros(values.shape, jnp.float32)
    for offset in range(kernel_width):
        summed = summed + weights[offset] * joined[offset : offset + length]
    return summed


def block_terms(x_blk, b_blk, c_blk, dt_blk, log_blk):
    length = x_blk.shape[0]
    cumulative = jnp.cumsum(log_blk, axis=0)
    scores = jnp.dot(c_blk, b_blk.T, preferred_element_type=jnp.float32)
    log_gaps = cumulative[:, None, :] - cumulative[None, :, :]
    row_index = lax.broadcasted_iota(jnp.int32, (length, length), 0)
    col_index = lax.broadcasted_iota(jnp.int32, (length, length), 1)
    causal = (row_index >= col_index)[:, :, None]
    mixing = (
        scores[:, :, None] * jnp.exp(jnp.where(causal, log_gaps, -jnp.inf)) * dt_blk[None, :, :]
    ).astype(jnp.bfloat16)
    inside = jnp.einsum("ijh,jhp->ihp", mixing, x_blk, preferred_element_type=jnp.float32)
    to_end = jnp.exp(cumulative[-1:, :] - cumulative) * dt_blk
    weighted = (x_blk.astype(jnp.float32) * to_end[:, :, None]).astype(jnp.bfloat16)
    block_state = jnp.einsum("jhp,jn->hpn", weighted, b_blk, preferred_element_type=jnp.float32)
    return (inside, block_state, cumulative)


def per_device(
    tokens, owner_slot, w_in, w_bc, w_dt, conv_x, conv_bc, dt_bias, decay_rate, d_skip, norm_gain
):
    seq_count = lax.axis_size("seq")
    head_count = lax.axis_size("head")
    tok_rows = tokens.shape[0]
    width = tokens.shape[1]
    capacity = 2 * tok_rows // seq_count
    heads_here = dt_bias.shape[0]
    columns = w_in.shape[2]
    head_size = columns // (2 * heads_here)
    nstate = w_bc.shape[1] // 2
    own_index = lax.axis_index("seq")
    own_weight = w_in[0]
    x_halves = (picked(own_weight, 0, head_size, 0), picked(own_weight, 1, head_size, 0))
    z_halves = (picked(own_weight, 0, head_size, 1), picked(own_weight, 1, head_size, 1))
    x_a, x_b = exchange_pair(x_halves)
    z_first, z_second, a_last, b_last = lax.optimization_barrier((*z_halves, x_a[2], x_b[2]))
    x_a, x_b = (x_a[0], x_a[1], a_last), (x_b[0], x_b[1], b_last)
    z_a, z_b = exchange_pair((z_first, z_second))
    modality = (owner_slot // capacity) % MODS

    def project(slots, bits):
        first = bits[0]
        own_mod = own_index % MODS
        next_mod = (own_index ^ first) % MODS
        products = [
            jnp.dot(tokens, slot, preferred_element_type=jnp.float32).astype(jnp.bfloat16)
            for slot in slots
        ]
        return jnp.where(
            (modality == own_mod)[:, None],
            products[0],
            jnp.where((modality == next_mod)[:, None], products[1], products[2]),
        )

    x_raw = jnp.concatenate([project(x_a, (1, 2)), project(x_b, (2, 1))], axis=1)
    z_gate = jnp.concatenate([project(z_a, (1, 2)), project(z_b, (2, 1))], axis=1)
    bc_raw = jnp.dot(tokens, w_bc, preferred_element_type=jnp.float32).astype(jnp.bfloat16)
    dt_raw = jnp.dot(tokens, w_dt, preferred_element_type=jnp.float32)
    x_rim, bc_rim = passed_along(
        (x_raw[tok_rows - KCONV + 1 :], bc_raw[tok_rows - KCONV + 1 :]), "seq", 1
    )
    x_conv = jax.nn.silu(causal_conv(x_raw, x_rim, conv_x)).astype(jnp.bfloat16)
    bc_conv = jax.nn.silu(causal_conv(bc_raw, bc_rim, conv_bc)).astype(jnp.bfloat16)
    steps_dt = jax.nn.softplus(dt_raw + dt_bias)
    log_decay = -steps_dt * decay_rate
    block_total = tok_rows // QB
    x_blocks = x_conv.reshape(block_total, QB, heads_here, head_size)
    b_blocks = bc_conv[:, :nstate].reshape(block_total, QB, nstate)
    c_blocks = bc_conv[:, nstate:].reshape(block_total, QB, nstate)
    inside, block_state, cumulative = jax.vmap(block_terms)(
        x_blocks,
        b_blocks,
        c_blocks,
        steps_dt.reshape(block_total, QB, heads_here),
        log_decay.reshape(block_total, QB, heads_here),
    )
    block_log = cumulative[:, -1, :]
    zero_state = jnp.zeros((heads_here, head_size, nstate), jnp.float32)
    device_state = zero_state
    entering_list = []
    for block in range(block_total):
        entering_list.append(device_state)
        device_state = device_state * jnp.exp(block_log[block])[:, None, None] + block_state[block]
    entering_local = jnp.stack(entering_list)
    prior_log = jnp.cumsum(block_log, axis=0) - block_log
    device_log = jnp.sum(block_log, axis=0)
    log_rows = [
        jnp.broadcast_to(part[:, None, None], (heads_here, 1, nstate))
        for part in split_three(device_log)
    ]
    payload = jnp.concatenate(
        [
            device_state,
            *log_rows,
            jnp.zeros((heads_here, 5, nstate), jnp.float32),
        ],
        axis=1,
    ).astype(jnp.bfloat16)
    gathered = lax.all_gather(payload[None], "seq", axis=0, tiled=True).astype(jnp.float32)
    piece = gathered[:, :, :head_size]
    all_logs = jnp.sum(gathered[:, :, head_size : head_size + 3, 0], axis=2)
    prefix = jnp.cumsum(all_logs, axis=0)
    own_prefix = lax.dynamic_index_in_dim(
        prefix, own_index, 0, keepdims=False
    ) - lax.dynamic_index_in_dim(all_logs, own_index, 0, keepdims=False)
    piece_rows = piece.shape[0]
    positions = jnp.arange(piece_rows, dtype=jnp.int32)
    log_gap = own_prefix[None, :] - prefix
    factor = jnp.exp(jnp.where((positions < own_index)[:, None], log_gap, -jnp.inf))
    incoming = jnp.sum(piece * factor[:, :, None, None], axis=0)
    entering = entering_local + incoming[None] * jnp.exp(prior_log)[:, :, None, None]
    within = lax.optimization_barrier(
        inside + d_skip[None, None, :, None] * x_blocks.astype(jnp.float32)
    )
    outside = jnp.exp(cumulative)[..., None] * jnp.einsum(
        "bin,bhpn->bihp", c_blocks.astype(jnp.float32), entering, precision=PRECISE
    )
    outputs = within + outside
    outputs = outputs.reshape(tok_rows, heads_here * head_size)
    gated = outputs * jax.nn.silu(z_gate.astype(jnp.float32))
    squares = lax.psum(jnp.sum(gated * gated, axis=1), "head")
    inner_total = heads_here * head_size * head_count
    scaling = lax.rsqrt(squares / inner_total + EPSILON)
    return (gated * scaling[:, None] * norm_gain).astype(jnp.bfloat16)


def solution(mesh):
    return jax.shard_map(
        per_device,
        mesh=mesh,
        in_specs=(
            P("seq", None),
            P("seq"),
            P("seq", None, "head"),
            P(),
            P(None, "head"),
            P(None, "head"),
            P(),
            P("head"),
            P("head"),
            P("head"),
            P("head"),
        ),
        out_specs=P("seq", "head"),
        check_vma=False,
    )
```

```python
import jax
import jax.numpy as jnp
from jax import lax
from jax.sharding import PartitionSpec as P

KCONV = 4
QB = 256
MODS = 3


EPSILON = 1e-05
PRECISE = lax.Precision.HIGHEST


def passed_along(value, axis, steps):
    count = lax.axis_size(axis)
    initial, last = (max(0, -steps), min(count, count - steps))
    return lax.ppermute(value, axis, [(source, source + steps) for source in range(initial, last)])


def swapped(value, bit):
    count = lax.axis_size("seq")
    return lax.ppermute(value, "seq", [(source, source ^ bit) for source in range(count)])


def picked(weight, part, head_size, kind):
    columns = weight.shape[1] // 2
    source = lax.broadcasted_iota(jnp.int32, (columns, columns // 2), 0)
    target = lax.broadcasted_iota(jnp.int32, (columns, columns // 2), 1)
    wanted = (target // head_size) * 2 * head_size + kind * head_size + target % head_size
    chooser = (source == wanted).astype(jnp.bfloat16)
    chunk = weight[:, part * columns : (part + 1) * columns]
    return jnp.dot(chunk, chooser, preferred_element_type=jnp.float32).astype(jnp.bfloat16)


def split_three(value):
    high = lax.reduce_precision(value, 8, 7)
    middle = lax.reduce_precision(value - high, 8, 7)
    return high, middle, value - high - middle


def exchange_pair(halves):
    index = lax.axis_index("seq")
    orders = ((1, 2), (2, 1))
    firsts = [swapped(half, bits[0]) for half, bits in zip(halves, orders)]
    slots = []
    for half, got, bits in zip(halves, firsts, orders):
        partner = index ^ bits[1]
        wanted = MODS - partner % MODS - (partner ^ bits[0]) % MODS
        sent = jnp.where(index % MODS == wanted, half, got)
        slots.append((half, got, swapped(sent, bits[1])))
    return slots


def causal_conv(values, rim, weights):
    kernel_width = weights.shape[0]
    joined = jnp.concatenate([rim, values]).astype(jnp.float32)
    length = values.shape[0]
    summed = jnp.zeros(values.shape, jnp.float32)
    for offset in range(kernel_width):
        summed = summed + weights[offset] * joined[offset : offset + length]
    return summed


def block_terms(x_blk, b_blk, c_blk, dt_blk, log_blk):
    length = x_blk.shape[0]
    cumulative = jnp.cumsum(log_blk, axis=0)
    scores = jnp.dot(c_blk, b_blk.T, preferred_element_type=jnp.float32)
    log_gaps = cumulative[:, None, :] - cumulative[None, :, :]
    row_index = lax.broadcasted_iota(jnp.int32, (length, length), 0)
    col_index = lax.broadcasted_iota(jnp.int32, (length, length), 1)
    causal = (row_index >= col_index)[:, :, None]
    mixing = (
        scores[:, :, None] * jnp.exp(jnp.where(causal, log_gaps, -jnp.inf)) * dt_blk[None, :, :]
    ).astype(jnp.bfloat16)
    inside = jnp.einsum("ijh,jhp->ihp", mixing, x_blk, preferred_element_type=jnp.float32)
    to_end = jnp.exp(cumulative[-1:, :] - cumulative) * dt_blk
    weighted = (x_blk.astype(jnp.float32) * to_end[:, :, None]).astype(jnp.bfloat16)
    block_state = jnp.einsum("jhp,jn->hpn", weighted, b_blk, preferred_element_type=jnp.float32)
    return (inside, block_state, cumulative)


def per_device(
    tokens, owner_slot, w_in, w_bc, w_dt, conv_x, conv_bc, dt_bias, decay_rate, d_skip, norm_gain
):
    seq_count = lax.axis_size("seq")
    head_count = lax.axis_size("head")
    tok_rows = tokens.shape[0]
    width = tokens.shape[1]
    capacity = 2 * tok_rows // seq_count
    heads_here = dt_bias.shape[0]
    columns = w_in.shape[2]
    head_size = columns // (2 * heads_here)
    nstate = w_bc.shape[1] // 2
    own_index = lax.axis_index("seq")
    own_weight = w_in[0]
    x_halves = (picked(own_weight, 0, head_size, 0), picked(own_weight, 1, head_size, 0))
    z_halves = (picked(own_weight, 0, head_size, 1), picked(own_weight, 1, head_size, 1))
    x_a, x_b = exchange_pair(x_halves)
    z_first, z_second, a_got, b_got = lax.optimization_barrier((*z_halves, x_a[1], x_b[1]))
    x_a, x_b = (x_a[0], a_got, x_a[2]), (x_b[0], b_got, x_b[2])
    z_a, z_b = exchange_pair((z_first, z_second))
    modality = (owner_slot // capacity) % MODS

    def project(slots, bits):
        first = bits[0]
        own_mod = own_index % MODS
        next_mod = (own_index ^ first) % MODS
        products = [
            jnp.dot(tokens, slot, preferred_element_type=jnp.float32).astype(jnp.bfloat16)
            for slot in slots
        ]
        return jnp.where(
            (modality == own_mod)[:, None],
            products[0],
            jnp.where((modality == next_mod)[:, None], products[1], products[2]),
        )

    x_raw = jnp.concatenate([project(x_a, (1, 2)), project(x_b, (2, 1))], axis=1)
    z_gate = jnp.concatenate([project(z_a, (1, 2)), project(z_b, (2, 1))], axis=1)
    bc_raw = jnp.dot(tokens, w_bc, preferred_element_type=jnp.float32).astype(jnp.bfloat16)
    dt_raw = jnp.dot(tokens, w_dt, preferred_element_type=jnp.float32)
    x_rim, bc_rim = passed_along(
        (x_raw[tok_rows - KCONV + 1 :], bc_raw[tok_rows - KCONV + 1 :]), "seq", 1
    )
    x_conv = jax.nn.silu(causal_conv(x_raw, x_rim, conv_x)).astype(jnp.bfloat16)
    bc_conv = jax.nn.silu(causal_conv(bc_raw, bc_rim, conv_bc)).astype(jnp.bfloat16)
    steps_dt = jax.nn.softplus(dt_raw + dt_bias)
    log_decay = -steps_dt * decay_rate
    block_total = tok_rows // QB
    x_blocks = x_conv.reshape(block_total, QB, heads_here, head_size)
    b_blocks = bc_conv[:, :nstate].reshape(block_total, QB, nstate)
    c_blocks = bc_conv[:, nstate:].reshape(block_total, QB, nstate)
    inside, block_state, cumulative = jax.vmap(block_terms)(
        x_blocks,
        b_blocks,
        c_blocks,
        steps_dt.reshape(block_total, QB, heads_here),
        log_decay.reshape(block_total, QB, heads_here),
    )
    block_log = cumulative[:, -1, :]
    zero_state = jnp.zeros((heads_here, head_size, nstate), jnp.float32)
    device_state = zero_state
    entering_list = []
    for block in range(block_total):
        entering_list.append(device_state)
        device_state = device_state * jnp.exp(block_log[block])[:, None, None] + block_state[block]
    entering_local = jnp.stack(entering_list)
    prior_log = jnp.cumsum(block_log, axis=0) - block_log
    device_log = jnp.sum(block_log, axis=0)
    log_rows = [
        jnp.broadcast_to(part[:, None, None], (heads_here, 1, nstate))
        for part in split_three(device_log)
    ]
    payload = jnp.concatenate(
        [
            device_state,
            *log_rows,
            jnp.zeros((heads_here, 5, nstate), jnp.float32),
        ],
        axis=1,
    ).astype(jnp.bfloat16)
    gathered = lax.all_gather(payload[None], "seq", axis=0, tiled=True).astype(jnp.float32)
    piece = gathered[:, :, :head_size]
    all_logs = jnp.sum(gathered[:, :, head_size : head_size + 3, 0], axis=2)
    prefix = jnp.cumsum(all_logs, axis=0)
    own_prefix = lax.dynamic_index_in_dim(
        prefix, own_index, 0, keepdims=False
    ) - lax.dynamic_index_in_dim(all_logs, own_index, 0, keepdims=False)
    piece_rows = piece.shape[0]
    positions = jnp.arange(piece_rows, dtype=jnp.int32)
    log_gap = own_prefix[None, :] - prefix
    factor = jnp.exp(jnp.where((positions < own_index)[:, None], log_gap, -jnp.inf))
    incoming = jnp.sum(piece * factor[:, :, None, None], axis=0)
    entering = entering_local + incoming[None] * jnp.exp(prior_log)[:, :, None, None]
    within = lax.optimization_barrier(
        inside + d_skip[None, None, :, None] * x_blocks.astype(jnp.float32)
    )
    outside = jnp.exp(cumulative)[..., None] * jnp.einsum(
        "bin,bhpn->bihp", c_blocks.astype(jnp.float32), entering, precision=PRECISE
    )
    outputs = within + outside
    outputs = outputs.reshape(tok_rows, heads_here * head_size)
    gated = outputs * jax.nn.silu(z_gate.astype(jnp.float32))
    squares = lax.psum(jnp.sum(gated * gated, axis=1), "head")
    inner_total = heads_here * head_size * head_count
    scaling = lax.rsqrt(squares / inner_total + EPSILON)
    return (gated * scaling[:, None] * norm_gain).astype(jnp.bfloat16)


def solution(mesh):
    return jax.shard_map(
        per_device,
        mesh=mesh,
        in_specs=(
            P("seq", None),
            P("seq"),
            P("seq", None, "head"),
            P(),
            P(None, "head"),
            P(None, "head"),
            P(),
            P("head"),
            P("head"),
            P("head"),
            P("head"),
        ),
        out_specs=P("seq", "head"),
        check_vma=False,
    )
```
